512 devices in a mesh: samp: 64 (over z, y), mark: 8 (over x, core).
Axes of the slice: x: 4, y: 8, z: 8, core: 2. Of those that a mesh axis runs over, the one named last changes fastest.
Arguments:
- dosage: bfloat16 [32768, 2048], P('samp', 'mark'), may hold values from 0 to 2
- alt_count: int32 [2048], P('mark'), may hold values from 40000 to 759999
- obs_count: int32 [2048], P('mark'), may hold values from 400000 to 500000
- sample_weight: float32 [32768], P('samp'), may hold values from 0.25 to 12, as said below
- test_matrix: bfloat16 [2048, 256], P(('mark', 'samp')), may hold values from -6 to 6
Outputs:
- basis: float32 [32768, 256], P(('samp', 'mark'))
- loadings: float32 [2048, 256], P(('mark', 'samp'))
The draws below stay inside these ranges and needn't reach their ends.
Inputs may be any that keep to these rules, and one draw needn't show every extreme that they name: `sample_weight`: every weight is positive.
All inputs are finite; a program needn't handle non-finite values.
Results may differ from the reference program's by a relative error of at most 0.004.
Values may be sent and summed in bfloat16 or wider, within the bound.
A program may use at most 64 MiB of HBM per device.

```python
import math
import jax
import jax.numpy as jnp
from jax import lax

K = 256
RS = 512
NS = 32768
NM = 2048
N_SAMP = 64


def draw_sample_weight(key, part):
    position = jnp.arange(NS, dtype=jnp.float32)
    rising = 1.0 + 2.0 * position / (NS - 1)
    jitter = jnp.exp(jax.random.uniform(key, (NS,), jnp.float32, -math.log(4.0), math.log(4.0)))
    return rising * jitter


def with_ends(values, own_key, low, high):
    longest = values.shape.index(max(values.shape))
    spots = []
    for shift in (0, 1):
        where = [jax.random.randint(jax.random.fold_in(own_key, axis), (), 0, length) for axis, length in enumerate(values.shape)]
        where[longest] = (where[longest] + shift) % values.shape[longest]
        spots.append(tuple(where))
    return values.at[spots[0]].set(low).at[spots[1]].set(high)


def levels(stream_key, dims, split, smallest, high):
    def one(axis_at, shards_of):
        heights = jax.random.uniform(jax.random.fold_in(jax.random.fold_in(stream_key, 6), axis_at), (shards_of,), jnp.float32, smallest / len(split), high / len(split))
        return jnp.repeat(jnp.exp(heights), dims[axis_at] // shards_of).reshape((-1,) + (1,) * (len(dims) - axis_at - 1))

    level = one(*split[0])
    for cut in split[1:]:
        level = level * one(*cut)
    return level


def scatter_about(own_key, dims, deviation, most, split=(), kind=jnp.bfloat16):
    gain = levels(own_key, dims, split, -0.22, 0.18) if split else 1.0
    entries = jax.random.normal(own_key, dims, jnp.float32) * deviation * gain
    return jnp.minimum(jnp.maximum(entries, -most), most).astype(kind)


def setup_inputs(seed: int = 0) -> dict:
    key_of = jax.random.split(jax.random.key(seed), 6)
    dosage = jnp.clip(2.0 * jax.random.uniform(key_of[0], (NS, NM), jnp.float32) ** levels(key_of[0], (NS, NM), ((0, 64), (1, 8)), -0.2, 0.2), 0.0, 2.0).astype(jnp.bfloat16)
    alt_count = with_ends(jax.random.randint(key_of[1], (NM,), 40000, 760000), jax.random.fold_in(key_of[1], 1), 40000, 759999).astype(jnp.int32)
    obs_count = with_ends(jax.random.randint(key_of[2], (NM,), 400000, 500001), jax.random.fold_in(key_of[2], 1), 400000, 500000).astype(jnp.int32)
    sample_weight = draw_sample_weight(jax.random.fold_in(key_of[5], 71), 0)
    test_matrix = scatter_about(key_of[4], (NM, K), 1.0, 6.0, ((0, 512),))
    return dict(dosage=dosage, alt_count=alt_count, obs_count=obs_count, sample_weight=sample_weight, test_matrix=test_matrix)


def standardize(block, weights, freq, scale):
    return (jnp.sqrt(weights)[:, None] * (block.astype(jnp.float32) - 2.0 * freq) * scale).astype(jnp.bfloat16)

def reference(dosage, alt_count, obs_count, sample_weight, test_matrix):
    freq = alt_count.astype(jnp.float32) / (2.0 * obs_count.astype(jnp.float32))
    scale = 1.0 / jnp.sqrt(2.0 * freq * (1.0 - freq))
    blocks = dosage.reshape(N_SAMP, RS, NM)
    weight_blocks = sample_weight.reshape(N_SAMP, RS)

    def sketch_block(pair):
        standard = standardize(pair[0], pair[1], freq, scale)
        return jnp.dot(standard.astype(jnp.float32), test_matrix.astype(jnp.float32), preferred_element_type=jnp.float32)
    sketch = lax.map(sketch_block, (blocks, weight_blocks)).reshape(NS, K)
    gram = lax.dot_general(sketch.astype(jnp.float32), sketch.astype(jnp.float32), (((0,), (0,)), ((), ())), precision=lax.Precision.HIGHEST, preferred_element_type=jnp.float32)
    lower = jnp.linalg.cholesky(gram)
    basis = math.sqrt(NS) * lax.linalg.triangular_solve(lower, sketch, left_side=False, lower=True, transpose_a=True)
    sketch_round = sketch.astype(jnp.bfloat16).reshape(N_SAMP, RS, K)

    def project_block(total, triple):
        standard = standardize(triple[0], triple[1], freq, scale)
        term = lax.dot_general(standard.astype(jnp.float32), triple[2].astype(jnp.float32), (((0,), (0,)), ((), ())), preferred_element_type=jnp.float32)
        return (total + term, None)
    projected, unused = lax.scan(project_block, jnp.zeros((NM, K), jnp.float32), (blocks, weight_blocks, sketch_round))
    loadings = lax.linalg.triangular_solve(lower, projected, left_side=False, lower=True, transpose_a=True)
    return (basis, loadings)
```

```python
import functools
import math

import jax
import jax.numpy as jnp
from jax import lax
from jax.experimental import pallas as pl
from jax.experimental.pallas import tpu as pltpu
from jax.sharding import PartitionSpec as P

F32 = jnp.float32
BF16 = jnp.bfloat16
RING = 8
XS = 4
CORES = 2
MARKS = XS * CORES
FAR_RING = (4, 3, 5, 2, 6, 1, 7)
FAR_X = (2, 1, 3)
HIGHEST = lax.Precision.HIGHEST


def inverse_factor(groups):
    lane = lax.broadcasted_iota(jnp.int32, (8, 128), 1)
    row = lax.broadcasted_iota(jnp.int32, (8, 128), 0)
    rows = list(groups)
    count = len(rows)
    for b in range(count):
        start = 8 * b
        inside = (lane >= start) & (lane < start + 8)
        cols = {
            g: [jnp.broadcast_to(rows[g][:, start + j : start + j + 1], (8, 128)) for j in range(8)]
            for g in range(b, count)
        }
        panel = jnp.where(inside, jnp.where(lane - start == row, 1.0, 0.0), rows[b])
        own = cols[b]
        scaled, roots, upper = [], [], {}
        for k in range(8):
            root = lax.rsqrt(jnp.broadcast_to(own[k][k : k + 1], (8, 128)))
            line = jnp.broadcast_to(panel[k : k + 1], (8, 128)) * root
            below = jnp.where(row > k, own[k] * root, 0.0)
            panel = jnp.where(row == k, line, panel - below * line)
            for j in range(k + 1, 8):
                upper[k, j] = jnp.broadcast_to(own[j][k : k + 1], (8, 128)) * root
                own[j] = own[j] - below * upper[k, j]
            scaled.append(line)
            roots.append(root)
        rows[b] = panel
        for g in range(b + 1, count):
            left = jnp.where(inside, 0.0, rows[g])
            theirs = cols[g]
            for k in range(8):
                factor = theirs[k] * roots[k]
                left = left - factor * scaled[k]
                for j in range(k + 1, 8):
                    theirs[j] = theirs[j] - factor * upper[k, j]
            rows[g] = left
    return [jnp.where(lane <= row + 8 * g, rows[g], 0.0) for g in range(count)]


def dot_t(a, b):
    return lax.dot_general(a, b, (((1,), (1,)), ((), ())), precision=HIGHEST, preferred_element_type=F32)


def dot_cols(a, b):
    return lax.dot_general(a, b, (((0,), (0,)), ((), ())), preferred_element_type=F32)


def kernel(
    total,
    dosage_hbm, counts_ref, weight_ref, test_hbm,
    basis_ref, loadings_ref,
    dosage, std, ta, tb, tfull, tbf,
    pair_out, pair_in, sk_out, sk_in, sketch, yr,
    gs, ga, gb, ha, hb, gf, inv,
    pv, pz, ps, py,
    in_sem,
    t1s, t1r, t2s, t2r, prs, prr, sks, skr, yxs, yxr, yps, ypr,
    g1s, g1r, g2s, g2r, fxs, fxr, fps, fpr, z1s, z1r, y1s, y1r,
):
    samp, mark = lax.axis_index("samp"), lax.axis_index("mark")
    z, y = samp // RING, samp % RING
    x, c = mark // CORES, mark % CORES
    partner = (samp, x * CORES + (1 - c))

    def at_y(d):
        return (z * RING + (y + d) % RING, mark)

    def at_z(d):
        return (((z + d) % RING) * RING + y, mark)

    def at_x(d):
        return (samp, ((x + d) % XS) * CORES + c)

    def push(src, dst, send, recv, to):
        copy = pltpu.make_async_remote_copy(
            src_ref=src, dst_ref=dst, send_sem=send, recv_sem=recv,
            device_id=to, device_id_type=pl.DeviceIdType.MESH,
        )
        copy.start()
        return copy

    started = []

    own_a = pltpu.make_async_copy(test_hbm.at[:, pl.ds(0, 128)], ta.at[z, y], in_sem.at[0])
    own_b = pltpu.make_async_copy(test_hbm.at[:, pl.ds(128, 128)], tb.at[y, z], in_sem.at[1])
    own_d = pltpu.make_async_copy(dosage_hbm, dosage, in_sem.at[2])
    own_a.start()
    own_b.start()
    own_d.start()

    barrier = pltpu.get_barrier_semaphore()
    peers = [at_y(d) for d in FAR_RING] + [at_z(d) for d in FAR_RING] + [at_x(d) for d in FAR_X] + [partner]
    for peer in peers:
        pl.semaphore_signal(barrier, inc=1, device_id=peer, device_id_type=pl.DeviceIdType.MESH)
    own_a.wait()
    own_b.wait()
    pl.semaphore_wait(barrier, len(peers))

    first = []
    for d in FAR_RING:
        first.append(push(ta.at[z, y], ta.at[z, y], t1s.at[0, d - 1], t1r.at[0, d - 1], at_y(d)))
        first.append(push(tb.at[y, z], tb.at[y, z], t1s.at[1, d - 1], t1r.at[1, d - 1], at_z(d)))

    own_d.wait()
    alt = counts_ref[0:1].astype(F32)
    obs = counts_ref[1:2].astype(F32)
    freq = alt / (2.0 * obs)
    scale = 1.0 / jnp.sqrt(2.0 * freq * (1.0 - freq))
    roots = jnp.sqrt(weight_ref[...])
    tall = jnp.concatenate([roots] * 2, axis=0).T
    for q in range(4):
        rows = pl.ds(128 * q, 128)
        weights = jnp.broadcast_to(tall[:, q : q + 1], (128, 256))
        std[rows, :] = (weights * (dosage[rows, :].astype(F32) - 2.0 * freq) * scale).astype(BF16)

    for copy in first:
        copy.wait_recv()
    second = []
    for d in FAR_RING:
        second.append(push(ta.at[z], ta.at[z], t2s.at[0, d - 1], t2r.at[0, d - 1], at_z(d)))
        second.append(push(tb.at[y], tb.at[y], t2s.at[1, d - 1], t2r.at[1, d - 1], at_y(d)))
    for copy in second:
        copy.wait_recv()
    started += first + second
    for s in range(RING * RING):
        tfull[4 * s : 4 * s + 4, 0:128] = ta[s // RING, s % RING].astype(F32)
        tfull[4 * s : 4 * s + 4, 128:256] = tb[s % RING, s // RING].astype(F32)
    tbf[...] = tfull[...].astype(BF16)

    def partial_rows(owner):
        rows = pl.ds(pl.multiple_of(owner * 64, 64), 64)
        return jnp.dot(std[rows, :], tbf[...], preferred_element_type=F32)

    pair = {}
    for d in (2, 1, 3, 0):
        pair_out[d] = partial_rows(((x + d) % XS) * CORES + (1 - c))
        pair[d] = push(pair_out.at[d], pair_in.at[d], prs.at[d], prr.at[d], partner)
    mine = {d: partial_rows(((x + d) % XS) * CORES + c) for d in (2, 1, 3, 0)}
    along = {}
    for d in (2, 1, 3):
        pair[d].wait_recv()
        sk_out[d] = mine[d] + pair_in[d]
        along[d] = push(sk_out.at[d], sk_in.at[d], sks.at[d], skr.at[d], at_x(d))
    pair[0].wait_recv()
    own_sketch = mine[0] + pair_in[0]
    for d in (1, 3, 2):
        along[d].wait_recv()
        own_sketch = own_sketch + sk_in[d]
    sketch[...] = own_sketch
    started += list(pair.values()) + list(along.values())

    def gather_over_mark(buf, xs, xr, ps_, pr_):
        out = {d: push(buf.at[mark], buf.at[mark], xs.at[d], xr.at[d], at_x(d)) for d in FAR_X}
        over = {0: push(buf.at[mark], buf.at[mark], ps_.at[0], pr_.at[0], partner)}
        for d in (1, 3, 2):
            out[d].wait_recv()
            slot = ((x + XS - d) % XS) * CORES + c
            over[d] = push(buf.at[slot], buf.at[slot], ps_.at[d], pr_.at[d], partner)
        for d in (0, 1, 3, 2):
            over[d].wait_recv()
        started.extend(list(out.values()) + list(over.values()))

    yr[mark] = own_sketch.astype(BF16)
    gather_over_mark(yr, yxs, yxr, yps, ypr)
    rounded = yr[...].reshape(512, 256)

    left = dot_cols(rounded, rounded[:, 0:128])
    gs[0:256, :] = left
    gs[256:384, :] = dot_cols(rounded[:, 128:256], rounded[:, 128:256])
    part = pl.multiple_of(mark * 48, 8)
    ga[y] = gs[pl.ds(part, 24), :]
    gb[z] = gs[pl.ds(pl.multiple_of(part + 24, 8), 24), :]
    first = []
    for d in FAR_RING:
        first.append(push(ga.at[y], ga.at[y], g1s.at[0, d - 1], g1r.at[0, d - 1], at_y(d)))
        first.append(push(gb.at[z], gb.at[z], g1s.at[1, d - 1], g1r.at[1, d - 1], at_z(d)))

    pv[...] = dot_cols(std[...], rounded).reshape(RING, 32, 256)

    for copy in first:
        copy.wait_recv()
    ha[z] = jnp.sum(ga[...], axis=0)
    hb[y] = jnp.sum(gb[...], axis=0)
    second = []
    for d in FAR_RING:
        second.append(push(ha.at[z], ha.at[z], g2s.at[0, d - 1], g2r.at[0, d - 1], at_z(d)))
        second.append(push(hb.at[y], hb.at[y], g2s.at[1, d - 1], g2r.at[1, d - 1], at_y(d)))
    zsum = {}
    for d in FAR_RING:
        zsum[d] = push(pv.at[(z + d) % RING], pz.at[d], z1s.at[d], z1r.at[d], at_z(d))
    for copy in second:
        copy.wait_recv()
    started += first + second
    gf[mark] = jnp.concatenate([jnp.sum(ha[...], axis=0), jnp.sum(hb[...], axis=0)], axis=0)
    gather_over_mark(gf, fxs, fxr, fps, fpr)
    gs[...] = gf[...].reshape(384, 128)

    one = inverse_factor([gs[8 * g : 8 * g + 8, :] for g in range(16)])
    for g in range(16):
        inv[0, 8 * g : 8 * g + 8, :] = one[g]
    inv1 = inv[0]
    low = dot_t(gs[128:256, :], inv1)
    gs[256:384, :] = gs[256:384, :] - dot_t(low, low)

    psum = pv[z]
    for d in range(1, RING):
        zsum[d].wait_recv()
        psum = psum + pz[d]
    for q in range(RING):
        ps[q] = psum[4 * q : 4 * q + 4, :]
    ysum = {d: push(ps.at[(y + d) % RING], py.at[d], y1s.at[d], y1r.at[d], at_y(d)) for d in FAR_RING}
    started += list(zsum.values()) + list(ysum.values())

    two = inverse_factor([gs[256 + 8 * g : 264 + 8 * g, :] for g in range(16)])
    for g in range(16):
        inv[1, 8 * g : 8 * g + 8, :] = two[g]
    inv2 = inv[1]

    own_sketch = sketch[...]
    head = dot_t(own_sketch[:, 0:128], inv1)
    tail = dot_t(own_sketch[:, 128:256] - dot_t(head, low), inv2)
    basis_ref[:, 0:128] = math.sqrt(total) * head
    basis_ref[:, 128:256] = math.sqrt(total) * tail

    projected = ps[y]
    for d in range(1, RING):
        ysum[d].wait_recv()
        projected = projected + py[d]
    projected = jnp.concatenate([projected, projected], axis=0)
    head = dot_t(projected[:, 0:128], inv1)
    tail = dot_t(projected[:, 128:256] - dot_t(head, low), inv2)
    loadings_ref[:, 0:128] = head[0:4]
    loadings_ref[:, 128:256] = tail[0:4]

    for copy in started:
        copy.wait_send()


def per_device(dosage, alt_count, obs_count, sample_weight, test_matrix):
    counts = jnp.stack([alt_count, obs_count])
    weights = sample_weight.reshape(4, 128)
    total = dosage.shape[0] * lax.axis_size("samp")
    dma = pltpu.SemaphoreType.DMA
    vmem = pl.BlockSpec(memory_space=pltpu.VMEM)
    hbm = pl.BlockSpec(memory_space=pl.ANY)
    two_rings = [dma((2, RING - 1))] * 2
    return pl.pallas_call(
        functools.partial(kernel, total),
        out_shape=(
            jax.ShapeDtypeStruct((64, 256), F32),
            jax.ShapeDtypeStruct((4, 256), F32),
        ),
        in_specs=[hbm, vmem, vmem, hbm],
        out_specs=(vmem, vmem),
        scratch_shapes=[
            pltpu.VMEM((512, 256), BF16),
            pltpu.VMEM((512, 256), BF16),
            pltpu.VMEM((RING, RING, 4, 128), BF16),
            pltpu.VMEM((RING, RING, 4, 128), BF16),
            pltpu.VMEM((256, 256), F32),
            pltpu.VMEM((256, 256), BF16),
            pltpu.VMEM((XS, 64, 256), F32),
            pltpu.VMEM((XS, 64, 256), F32),
            pltpu.VMEM((XS, 64, 256), F32),
            pltpu.VMEM((XS, 64, 256), F32),
            pltpu.VMEM((64, 256), F32),
            pltpu.VMEM((MARKS, 64, 256), BF16),
            pltpu.VMEM((384, 128), F32),
            pltpu.VMEM((RING, 24, 128), F32),
            pltpu.VMEM((RING, 24, 128), F32),
            pltpu.VMEM((RING, 24, 128), F32),
            pltpu.VMEM((RING, 24, 128), F32),
            pltpu.VMEM((MARKS, 48, 128), F32),
            pltpu.VMEM((2, 128, 128), F32),
            pltpu.VMEM((RING, 32, 256), F32),
            pltpu.VMEM((RING, 32, 256), F32),
            pltpu.VMEM((RING, 4, 256), F32),
            pltpu.VMEM((RING, 4, 256), F32),
            dma((3,)),
            *two_rings, *two_rings,
            *[dma((XS,))] * 8,
            *two_rings, *two_rings,
            *[dma((XS,))] * 4,
            *[dma((RING,))] * 4,
        ],
        compiler_params=pltpu.CompilerParams(collective_id=0, has_side_effects=True),
    )(dosage, counts, weights, test_matrix)


def solution(mesh):
    return jax.shard_map(
        per_device,
        mesh=mesh,
        in_specs=(P("samp", "mark"), P("mark"), P("mark"), P("samp"), P(("mark", "samp"), None)),
        out_specs=(P(("samp", "mark"), None), P(("mark", "samp"), None)),
        check_vma=False,
    )
```

```python
import functools
import math

import jax
import jax.numpy as jnp
from jax import lax
from jax.experimental import pallas as pl
from jax.experimental.pallas import tpu as pltpu
from jax.sharding import PartitionSpec as P

F32 = jnp.float32
BF16 = jnp.bfloat16
RING = 8
XS = 4
CORES = 2
MARKS = XS * CORES
FAR_RING = (4, 3, 5, 2, 6, 1, 7)
FAR_X = (2, 1, 3)
HIGHEST = lax.Precision.HIGHEST


def spread(column):
    return jnp.broadcast_to(column, (8, 128))


def inverse_factor(groups):
    lane = lax.broadcasted_iota(jnp.int32, (8, 128), 1)
    row = lax.broadcasted_iota(jnp.int32, (8, 128), 0)
    rows = list(groups)
    count = len(rows)
    own = [spread(rows[0][:, j : j + 1]) for j in range(8)]
    for b in range(count):
        start = 8 * b
        inside = (lane >= start) & (lane < start + 8)
        cols = {g: [spread(rows[g][:, start + j : start + j + 1]) for j in range(8)] for g in range(b + 1, count)}
        last = b + 1 == count
        following = None if last else [spread(rows[b + 1][:, start + 8 + j : start + 9 + j]) for j in range(8)]
        panel = jnp.where(inside, jnp.where(lane - start == row, 1.0, 0.0), rows[b])
        scaled, roots, upper, near = [], [], {}, []
        for k in range(8):
            root = lax.rsqrt(spread(own[k][k : k + 1]))
            line = spread(panel[k : k + 1]) * root
            below = own[k] * root
            for j in range(k + 1, 8):
                upper[k, j] = spread(own[j][k : k + 1]) * root
                own[j] = own[j] - below * upper[k, j]
            panel = jnp.where(row == k, line, panel - jnp.where(row > k, below, 0.0) * line)
            scaled.append(line)
            roots.append(root)
            if not last:
                theirs = cols[b + 1]
                factor = theirs[k] * root
                for j in range(k + 1, 8):
                    theirs[j] = theirs[j] - factor * upper[k, j]
                for j in range(8):
                    following[j] = following[j] - factor * spread(factor[j : j + 1])
                near.append(factor)
        rows[b] = panel
        for g in range(b + 1, count):
            left = jnp.where(inside, 0.0, rows[g])
            theirs = cols[g]
            for k in range(8):
                if g == b + 1:
                    factor = near[k]
                else:
                    factor = theirs[k] * roots[k]
                    for j in range(k + 1, 8):
                        theirs[j] = theirs[j] - factor * upper[k, j]
                left = left - factor * scaled[k]
            rows[g] = left
        own = following
    return [jnp.where(lane <= row + 8 * g, rows[g], 0.0) for g in range(count)]


def dot_t(a, b):
    return lax.dot_general(a, b, (((1,), (1,)), ((), ())), precision=HIGHEST, preferred_element_type=F32)


def dot_cols(a, b):
    return lax.dot_general(a, b, (((0,), (0,)), ((), ())), preferred_element_type=F32)


def kernel(
    total,
    dosage_hbm, alt_hbm, obs_hbm, weight_hbm, test_hbm,
    basis_ref, loadings_ref,
    dosage, alt, obs, weight, std, ta, tb, tfull, tbf,
    pair_out, pair_in, sk_out, sk_in, sketch, yr,
    gs, ga, gb, ha, hb, gf, inv,
    pv, pz, ps, py,
    in_sem,
    t1s, t1r, t2s, t2r, prs, prr, sks, skr, yxs, yxr, yps, ypr,
    g1s, g1r, g2s, g2r, fxs, fxr, fps, fpr, z1s, z1r, y1s, y1r,
):
    samp, mark = lax.axis_index("samp"), lax.axis_index("mark")
    z, y = samp // RING, samp % RING
    x, c = mark // CORES, mark % CORES
    partner = (samp, x * CORES + (1 - c))

    def at_y(d):
        return (z * RING + (y + d) % RING, mark)

    def at_z(d):
        return (((z + d) % RING) * RING + y, mark)

    def at_x(d):
        return (samp, ((x + d) % XS) * CORES + c)

    def push(src, dst, send, recv, to):
        copy = pltpu.make_async_remote_copy(
            src_ref=src, dst_ref=dst, send_sem=send, recv_sem=recv,
            device_id=to, device_id_type=pl.DeviceIdType.MESH,
        )
        copy.start()
        return copy

    started = []

    own_a = pltpu.make_async_copy(test_hbm.at[:, pl.ds(0, 128)], ta.at[z, y], in_sem.at[0])
    own_b = pltpu.make_async_copy(test_hbm.at[:, pl.ds(128, 128)], tb.at[y, z], in_sem.at[1])
    rest = [
        pltpu.make_async_copy(src, dst, in_sem.at[2 + i])
        for i, (src, dst) in enumerate(
            ((dosage_hbm, dosage), (alt_hbm, alt), (obs_hbm, obs), (weight_hbm, weight))
        )
    ]
    own_a.start()
    own_b.start()
    for copy in rest:
        copy.start()

    barrier = pltpu.get_barrier_semaphore()
    peers = [at_y(d) for d in FAR_RING] + [at_z(d) for d in FAR_RING] + [at_x(d) for d in FAR_X] + [partner]
    for peer in peers:
        pl.semaphore_signal(barrier, inc=1, device_id=peer, device_id_type=pl.DeviceIdType.MESH)
    own_a.wait()
    own_b.wait()
    pl.semaphore_wait(barrier, len(peers))

    first = []
    for d in FAR_RING:
        first.append(push(ta.at[z, y], ta.at[z, y], t1s.at[0, d - 1], t1r.at[0, d - 1], at_y(d)))
        first.append(push(tb.at[y, z], tb.at[y, z], t1s.at[1, d - 1], t1r.at[1, d - 1], at_z(d)))

    for copy in rest:
        copy.wait()
    freq = alt[...].astype(F32) / (2.0 * obs[...].astype(F32))
    scale = 1.0 / jnp.sqrt(2.0 * freq * (1.0 - freq))
    roots = jnp.sqrt(weight[...])
    tall = jnp.concatenate([roots] * 2, axis=0).T
    for q in range(4):
        rows = pl.ds(128 * q, 128)
        weights = jnp.broadcast_to(tall[:, q : q + 1], (128, 128))
        for h in range(2):
            cols = pl.ds(128 * h, 128)
            centred = dosage[rows, cols].astype(F32) - 2.0 * freq[h : h + 1]
            std[rows, cols] = (weights * centred * scale[h : h + 1]).astype(BF16)

    for copy in first:
        copy.wait_recv()
    second = []
    for d in FAR_RING:
        second.append(push(ta.at[z], ta.at[z], t2s.at[0, d - 1], t2r.at[0, d - 1], at_z(d)))
        second.append(push(tb.at[y], tb.at[y], t2s.at[1, d - 1], t2r.at[1, d - 1], at_y(d)))
    for copy in second:
        copy.wait_recv()
    started += first + second
    for s in range(RING * RING):
        tfull[4 * s : 4 * s + 4, 0:128] = ta[s // RING, s % RING].astype(F32)
        tfull[4 * s : 4 * s + 4, 128:256] = tb[s % RING, s // RING].astype(F32)
    tbf[...] = tfull[...].astype(BF16)

    def partial_rows(owner):
        rows = pl.ds(pl.multiple_of(owner * 64, 64), 64)
        return jnp.dot(std[rows, :], tbf[...], preferred_element_type=F32)

    pair = {}
    for d in (2, 1, 3, 0):
        pair_out[d] = partial_rows(((x + d) % XS) * CORES + (1 - c))
        pair[d] = push(pair_out.at[d], pair_in.at[d], prs.at[d], prr.at[d], partner)
    mine = {d: partial_rows(((x + d) % XS) * CORES + c) for d in (2, 1, 3, 0)}
    along = {}
    for d in (2, 1, 3):
        pair[d].wait_recv()
        sk_out[d] = mine[d] + pair_in[d]
        along[d] = push(sk_out.at[d], sk_in.at[d], sks.at[d], skr.at[d], at_x(d))
    pair[0].wait_recv()
    own_sketch = mine[0] + pair_in[0]
    for d in (1, 3, 2):
        along[d].wait_recv()
        own_sketch = own_sketch + sk_in[d]
    sketch[...] = own_sketch
    started += list(pair.values()) + list(along.values())

    def gather_over_mark(buf, xs, xr, ps_, pr_):
        out = {d: push(buf.at[mark], buf.at[mark], xs.at[d], xr.at[d], at_x(d)) for d in FAR_X}
        over = {0: push(buf.at[mark], buf.at[mark], ps_.at[0], pr_.at[0], partner)}
        for d in (1, 3, 2):
            out[d].wait_recv()
            slot = ((x + XS - d) % XS) * CORES + c
            over[d] = push(buf.at[slot], buf.at[slot], ps_.at[d], pr_.at[d], partner)
        for d in (0, 1, 3, 2):
            over[d].wait_recv()
        started.extend(list(out.values()) + list(over.values()))

    yr[mark] = own_sketch.astype(BF16)
    gather_over_mark(yr, yxs, yxr, yps, ypr)
    rounded = yr[...].reshape(512, 256)

    left = dot_cols(rounded, rounded[:, 0:128])
    gs[0:256, :] = left
    gs[256:384, :] = dot_cols(rounded[:, 128:256], rounded[:, 128:256])
    part = pl.multiple_of(mark * 48, 8)
    ga[y] = gs[pl.ds(part, 24), :]
    gb[z] = gs[pl.ds(pl.multiple_of(part + 24, 8), 24), :]
    first = []
    for d in FAR_RING:
        first.append(push(ga.at[y], ga.at[y], g1s.at[0, d - 1], g1r.at[0, d - 1], at_y(d)))
        first.append(push(gb.at[z], gb.at[z], g1s.at[1, d - 1], g1r.at[1, d - 1], at_z(d)))

    pv[...] = dot_cols(std[...], rounded).reshape(RING, 32, 256)

    for copy in first:
        copy.wait_recv()
    ha[z] = jnp.sum(ga[...], axis=0)
    hb[y] = jnp.sum(gb[...], axis=0)
    second = []
    for d in FAR_RING:
        second.append(push(ha.at[z], ha.at[z], g2s.at[0, d - 1], g2r.at[0, d - 1], at_z(d)))
        second.append(push(hb.at[y], hb.at[y], g2s.at[1, d - 1], g2r.at[1, d - 1], at_y(d)))
    zsum = {}
    for d in FAR_RING:
        zsum[d] = push(pv.at[(z + d) % RING], pz.at[d], z1s.at[d], z1r.at[d], at_z(d))
    for copy in second:
        copy.wait_recv()
    started += first + second
    gf[mark] = jnp.concatenate([jnp.sum(ha[...], axis=0), jnp.sum(hb[...], axis=0)], axis=0)
    gather_over_mark(gf, fxs, fxr, fps, fpr)
    gs[...] = gf[...].reshape(384, 128)

    psum = pv[z]
    for d in range(1, RING):
        zsum[d].wait_recv()
        psum = psum + pz[d]
    for q in range(RING):
        ps[q] = psum[4 * q : 4 * q + 4, :]
    ysum = {d: push(ps.at[(y + d) % RING], py.at[d], y1s.at[d], y1r.at[d], at_y(d)) for d in FAR_RING}
    started += list(zsum.values()) + list(ysum.values())

    one = inverse_factor([gs[8 * g : 8 * g + 8, :] for g in range(16)])
    for g in range(16):
        inv[0, 8 * g : 8 * g + 8, :] = one[g]
    inv1 = inv[0]
    low = dot_t(gs[128:256, :], inv1)
    gs[256:384, :] = gs[256:384, :] - dot_t(low, low)

    head = dot_t(sketch[:, 0:128], inv1)
    middle = sketch[:, 128:256] - dot_t(head, low)

    two = inverse_factor([gs[256 + 8 * g : 264 + 8 * g, :] for g in range(16)])
    for g in range(16):
        inv[1, 8 * g : 8 * g + 8, :] = two[g]
    inv2 = inv[1]
    projected = ps[y]
    for d in range(1, RING):
        ysum[d].wait_recv()
        projected = projected + py[d]
    projected = jnp.concatenate([projected, projected], axis=0)
    head_p = dot_t(projected[:, 0:128], inv1)
    middle_p = projected[:, 128:256] - dot_t(head_p, low)
    tail = dot_t(jnp.concatenate([middle, middle_p], axis=0), inv2)
    basis_ref[:, 0:128] = math.sqrt(total) * head
    basis_ref[:, 128:256] = math.sqrt(total) * tail[0:64]
    loadings_ref[:, 0:128] = head_p[0:4]
    loadings_ref[:, 128:256] = tail[64:68]

    for copy in started:
        copy.wait_send()


def hand_over(basis_in, loadings_in, basis_out, loadings_out, sems):
    copies = [
        pltpu.make_async_copy(basis_in, basis_out, sems.at[0]),
        pltpu.make_async_copy(loadings_in, loadings_out, sems.at[1]),
    ]
    for copy in copies:
        copy.start()
    for copy in copies:
        copy.wait()


def per_device(dosage, alt_count, obs_count, sample_weight, test_matrix):
    total = dosage.shape[0] * lax.axis_size("samp")
    dma = pltpu.SemaphoreType.DMA
    vmem = pl.BlockSpec(memory_space=pltpu.VMEM)
    hbm = pl.BlockSpec(memory_space=pltpu.HBM)
    two_rings = [dma((2, RING - 1))] * 2
    shapes = ((64, 256), F32), ((4, 256), F32)
    args = (
        dosage,
        alt_count.reshape(2, 128),
        obs_count.reshape(2, 128),
        sample_weight.reshape(4, 128),
        test_matrix,
    )
    basis, loadings = pl.pallas_call(
        functools.partial(kernel, total),
        out_shape=tuple(pltpu.VMEM(*s) for s in shapes),
        in_specs=[hbm] * 5,
        out_specs=(vmem, vmem),
        scratch_shapes=[
            pltpu.VMEM((512, 256), BF16),
            pltpu.VMEM((2, 128), jnp.int32),
            pltpu.VMEM((2, 128), jnp.int32),
            pltpu.VMEM((4, 128), F32),
            pltpu.VMEM((512, 256), BF16),
            pltpu.VMEM((RING, RING, 4, 128), BF16),
            pltpu.VMEM((RING, RING, 4, 128), BF16),
            pltpu.VMEM((256, 256), F32),
            pltpu.VMEM((256, 256), BF16),
            pltpu.VMEM((XS, 64, 256), F32),
            pltpu.VMEM((XS, 64, 256), F32),
            pltpu.VMEM((XS, 64, 256), F32),
            pltpu.VMEM((XS, 64, 256), F32),
            pltpu.VMEM((64, 256), F32),
            pltpu.VMEM((MARKS, 64, 256), BF16),
            pltpu.VMEM((384, 128), F32),
            pltpu.VMEM((RING, 24, 128), F32),
            pltpu.VMEM((RING, 24, 128), F32),
            pltpu.VMEM((RING, 24, 128), F32),
            pltpu.VMEM((RING, 24, 128), F32),
            pltpu.VMEM((MARKS, 48, 128), F32),
            pltpu.VMEM((2, 128, 128), F32),
            pltpu.VMEM((RING, 32, 256), F32),
            pltpu.VMEM((RING, 32, 256), F32),
            pltpu.VMEM((RING, 4, 256), F32),
            pltpu.VMEM((RING, 4, 256), F32),
            dma((6,)),
            *two_rings, *two_rings,
            *[dma((XS,))] * 8,
            *two_rings, *two_rings,
            *[dma((XS,))] * 4,
            *[dma((RING,))] * 4,
        ],
        compiler_params=pltpu.CompilerParams(
            collective_id=0, has_side_effects=True, vmem_limit_bytes=24 * 1024 * 1024
        ),
    )(*[pltpu.with_memory_space_constraint(arg, pltpu.HBM) for arg in args])
    return pl.pallas_call(
        hand_over,
        out_shape=tuple(jax.ShapeDtypeStruct(*s) for s in shapes),
        in_specs=[vmem] * 2,
        out_specs=(hbm, hbm),
        scratch_shapes=[dma((2,))],
        compiler_params=pltpu.CompilerParams(vmem_limit_bytes=1024 * 1024),
    )(basis, loadings)


def solution(mesh):
    return jax.shard_map(
        per_device,
        mesh=mesh,
        in_specs=(P("samp", "mark"), P("mark"), P("mark"), P("samp"), P(("mark", "samp"), None)),
        out_specs=(P(("samp", "mark"), None), P(("mark", "samp"), None)),
        check_vma=False,
    )
```

```python
import functools
import math

import jax
import jax.numpy as jnp
from jax import lax
from jax.experimental import pallas as pl
from jax.experimental.pallas import tpu as pltpu
from jax.sharding import PartitionSpec as P

F32 = jnp.float32
BF16 = jnp.bfloat16
RING = 8
XS = 4
CORES = 2
MARKS = XS * CORES
FAR_RING = (4, 3, 5, 2, 6, 1, 7)
FAR_X = (2, 1, 3)
HIGHEST = lax.Precision.HIGHEST


def spread(column):
    return jnp.broadcast_to(column, (8, 128))


def inverse_factor(groups, meanwhile=None):
    lane = lax.broadcasted_iota(jnp.int32, (8, 128), 1)
    row = lax.broadcasted_iota(jnp.int32, (8, 128), 0)
    rows = list(groups)
    count = len(rows)
    own = [spread(rows[0][:, j : j + 1]) for j in range(8)]
    for b in range(count):
        if meanwhile is not None and b in meanwhile:
            meanwhile[b]()
        start = 8 * b
        inside = (lane >= start) & (lane < start + 8)
        cols = {g: [spread(rows[g][:, start + j : start + j + 1]) for j in range(8)] for g in range(b + 1, count)}
        last = b + 1 == count
        following = None if last else [spread(rows[b + 1][:, start + 8 + j : start + 9 + j]) for j in range(8)]
        panel = jnp.where(inside, jnp.where(lane - start == row, 1.0, 0.0), rows[b])
        scaled, roots, upper, near = [], [], {}, []
        for k in range(8):
            root = lax.rsqrt(spread(own[k][k : k + 1]))
            line = spread(panel[k : k + 1]) * root
            below = own[k] * root
            for j in range(k + 1, 8):
                upper[k, j] = spread(own[j][k : k + 1]) * root
                own[j] = own[j] - below * upper[k, j]
            panel = jnp.where(row == k, line, panel - jnp.where(row > k, below, 0.0) * line)
            scaled.append(line)
            roots.append(root)
            if not last:
                theirs = cols[b + 1]
                factor = theirs[k] * root
                for j in range(k + 1, 8):
                    theirs[j] = theirs[j] - factor * upper[k, j]
                for j in range(8):
                    following[j] = following[j] - factor * spread(factor[j : j + 1])
                near.append(factor)
        rows[b] = panel
        for g in range(b + 1, count):
            left = jnp.where(inside, 0.0, rows[g])
            theirs = cols[g]
            for k in range(8):
                if g == b + 1:
                    factor = near[k]
                else:
                    factor = theirs[k] * roots[k]
                    for j in range(k + 1, 8):
                        theirs[j] = theirs[j] - factor * upper[k, j]
                left = left - factor * scaled[k]
            rows[g] = left
        own = following
    return [jnp.where(lane <= row + 8 * g, rows[g], 0.0) for g in range(count)]


def dot_t(a, b):
    return lax.dot_general(a, b, (((1,), (1,)), ((), ())), precision=HIGHEST, preferred_element_type=F32)


def dot_cols(a, b):
    return lax.dot_general(a, b, (((0,), (0,)), ((), ())), preferred_element_type=F32)


def kernel(
    total,
    dosage_hbm, alt_hbm, obs_hbm, weight_hbm, test_hbm,
    basis_ref, loadings_ref,
    dosage, alt, obs, weight, std, ta, tb, tfull, tbf,
    partial, pair_in, sk_out, sk_in, sketch, yr0, yr1,
    g1, g2, ga1, gb1, ha1, hb1, gf1, ga2, gb2, ha2, hb2, gf2, inv,
    pva, pvb, pza, pzb, psa, psb, pya, pyb, pm,
    in_sem,
    t1s, t1r, t2s, t2r, prs, prr, sks, skr, yxs, yxr, yps, ypr, y2s, y2r,
    g11s, g11r, g12s, g12r, g21s, g21r, g22s, g22r,
    fxs, fxr, f2s, f2r, z1s, z1r, y1s, y1r,
):
    samp, mark = lax.axis_index("samp"), lax.axis_index("mark")
    z, y = samp // RING, samp % RING
    x, c = mark // CORES, mark % CORES
    partner = (samp, x * CORES + (1 - c))

    def at_y(d):
        return (z * RING + (y + d) % RING, mark)

    def at_z(d):
        return (((z + d) % RING) * RING + y, mark)

    def at_x(d):
        return (samp, ((x + d) % XS) * CORES + c)

    def at_other(d):
        return (samp, ((x + d) % XS) * CORES + (1 - c))

    def push(src, dst, send, recv, to):
        copy = pltpu.make_async_remote_copy(
            src_ref=src, dst_ref=dst, send_sem=send, recv_sem=recv,
            device_id=to, device_id_type=pl.DeviceIdType.MESH,
        )
        copy.start()
        return copy

    started = []

    own_a = pltpu.make_async_copy(test_hbm.at[:, pl.ds(0, 128)], ta.at[z, y], in_sem.at[0])
    own_b = pltpu.make_async_copy(test_hbm.at[:, pl.ds(128, 128)], tb.at[y, z], in_sem.at[1])
    rest = [
        pltpu.make_async_copy(src, dst, in_sem.at[2 + i])
        for i, (src, dst) in enumerate(
            ((dosage_hbm, dosage), (alt_hbm, alt), (obs_hbm, obs), (weight_hbm, weight))
        )
    ]
    own_a.start()
    own_b.start()
    for copy in rest:
        copy.start()

    barrier = pltpu.get_barrier_semaphore()
    peers = [at_y(d) for d in FAR_RING] + [at_z(d) for d in FAR_RING] + [at_x(d) for d in FAR_X]
    peers += [at_other(d) for d in FAR_X] + [partner]
    for peer in peers:
        pl.semaphore_signal(barrier, inc=1, device_id=peer, device_id_type=pl.DeviceIdType.MESH)
    own_a.wait()
    own_b.wait()
    pl.semaphore_wait(barrier, len(peers))

    first = []
    for d in FAR_RING:
        first.append(push(ta.at[z, y], ta.at[z, y], t1s.at[0, d - 1], t1r.at[0, d - 1], at_y(d)))
        first.append(push(tb.at[y, z], tb.at[y, z], t1s.at[1, d - 1], t1r.at[1, d - 1], at_z(d)))

    for copy in rest:
        copy.wait()
    freq = alt[...].astype(F32) / (2.0 * obs[...].astype(F32))
    scale = 1.0 / jnp.sqrt(2.0 * freq * (1.0 - freq))
    roots = jnp.sqrt(weight[...])
    tall = jnp.concatenate([roots] * 2, axis=0).T
    for q in range(4):
        rows = pl.ds(128 * q, 128)
        weights = jnp.broadcast_to(tall[:, q : q + 1], (128, 128))
        for h in range(2):
            cols = pl.ds(128 * h, 128)
            centred = dosage[rows, cols].astype(F32) - 2.0 * freq[h : h + 1]
            std[rows, cols] = (weights * centred * scale[h : h + 1]).astype(BF16)

    for copy in first:
        copy.wait_recv()
    second = []
    for d in FAR_RING:
        second.append(push(ta.at[z], ta.at[z], t2s.at[0, d - 1], t2r.at[0, d - 1], at_z(d)))
        second.append(push(tb.at[y], tb.at[y], t2s.at[1, d - 1], t2r.at[1, d - 1], at_y(d)))
    for copy in second:
        copy.wait_recv()
    started += first + second
    for s in range(RING * RING):
        tfull[4 * s : 4 * s + 4, 0:128] = ta[s // RING, s % RING].astype(F32)
        tfull[4 * s : 4 * s + 4, 128:256] = tb[s % RING, s // RING].astype(F32)
    tbf[...] = tfull[...].astype(BF16)

    def block(d, core):
        return ((x + d) % XS) * CORES + core

    steps = [(h, d) for h in range(2) for d in (2, 1, 3, 0)]
    pair, along = {}, {}
    for h, d in steps:
        if d == 2:
            half = jnp.dot(std[...], tbf[:, 128 * h : 128 * h + 128], preferred_element_type=F32)
            partial[h] = half.reshape(MARKS, 64, 128)
        pair[h, d] = push(partial.at[h, block(d, 1 - c)], pair_in.at[h, d], prs.at[h, d], prr.at[h, d], partner)
    for h, d in steps:
        if d:
            pair[h, d].wait_recv()
            sk_out[h, d] = partial[h, block(d, c)] + pair_in[h, d]
            along[h, d] = push(sk_out.at[h, d], sk_in.at[h, d], sks.at[h, d], skr.at[h, d], at_x(d))
    started += list(pair.values()) + list(along.values())

    def own_half(h):
        pair[h, 0].wait_recv()
        value = partial[h, block(0, c)] + pair_in[h, 0]
        for d in (1, 3, 2):
            along[h, d].wait_recv()
            value = value + sk_in[h, d]
        sketch[:, 128 * h : 128 * h + 128] = value
        return value.astype(BF16)

    def to_all_marks(buf, sends, recvs):
        copies = [
            push(buf.at[mark], buf.at[mark], sends.at[k], recvs.at[k], to)
            for k, to in enumerate([at_other(d) for d in FAR_X] + [at_x(d) for d in FAR_X] + [partner])
        ]
        started.extend(copies)
        return copies

    yr0[mark] = own_half(0)
    out = {d: push(yr0.at[mark], yr0.at[mark], yxs.at[d], yxr.at[d], at_x(d)) for d in FAR_X}
    over = {0: push(yr0.at[mark], yr0.at[mark], yps.at[0], ypr.at[0], partner)}
    yr1[mark] = own_half(1)
    second_half = to_all_marks(yr1, y2s, y2r)
    for d in (1, 3, 2):
        out[d].wait_recv()
        slot = ((x + XS - d) % XS) * CORES + c
        over[d] = push(yr0.at[slot], yr0.at[slot], yps.at[d], ypr.at[d], partner)
    for d in (0, 1, 3, 2):
        over[d].wait_recv()
    started += list(out.values()) + list(over.values())

    rounded0 = yr0[...].reshape(512, 128)

    def to_rings(left, right, sems, there, back):
        (lslot, lto), (rslot, rto) = there, back
        copies = []
        for d in FAR_RING:
            copies.append(push(left.at[lslot], left.at[lslot], sems[0].at[0, d - 1], sems[1].at[0, d - 1], lto(d)))
            copies.append(push(right.at[rslot], right.at[rslot], sems[0].at[1, d - 1], sems[1].at[1, d - 1], rto(d)))
        started.extend(copies)
        return copies

    def arrived(copies):
        for copy in copies:
            copy.wait_recv()

    along_y, along_z = (y, at_y), (z, at_z)

    g1[...] = dot_cols(rounded0, rounded0)
    part = pl.multiple_of(mark * 16, 16)
    ga1[y] = g1[pl.ds(part, 8), :]
    gb1[z] = g1[pl.ds(pl.multiple_of(part + 8, 8), 8), :]
    first1 = to_rings(ga1, gb1, (g11s, g11r), along_y, along_z)
    arrived(second_half)
    rounded1 = yr1[...].reshape(512, 128)
    g2[0:128, :] = dot_cols(rounded1, rounded0)
    g2[128:256, :] = dot_cols(rounded1, rounded1)
    part = pl.multiple_of(mark * 32, 32)
    ga2[y] = g2[pl.ds(part, 16), :]
    gb2[z] = g2[pl.ds(pl.multiple_of(part + 16, 16), 16), :]
    first2 = to_rings(ga2, gb2, (g12s, g12r), along_y, along_z)

    pva[...] = dot_cols(std[...], rounded0).reshape(RING, 32, 128)
    pm[...] = dot_cols(std[...], rounded1)
    for q in range(RING * RING):
        pvb[q % RING, 4 * (q // RING) : 4 * (q // RING) + 4, :] = pm[4 * q : 4 * q + 4, :]

    pfirst = []

    def pass_on(distances):
        for d in distances:
            pfirst.append(push(pva.at[(z + d) % RING], pza.at[d], z1s.at[0, d - 1], z1r.at[0, d - 1], at_z(d)))
            pfirst.append(push(pvb.at[(y + d) % RING], pzb.at[d], z1s.at[1, d - 1], z1r.at[1, d - 1], at_y(d)))

    pass_on((3, 5, 2, 6, 1, 7))
    arrived(first1)
    ha1[z] = jnp.sum(ga1[...], axis=0)
    hb1[y] = jnp.sum(gb1[...], axis=0)
    second1 = to_rings(ha1, hb1, (g21s, g21r), along_z, along_y)
    pass_on((4,))
    arrived(first2)
    ha2[z] = jnp.sum(ga2[...], axis=0)
    hb2[y] = jnp.sum(gb2[...], axis=0)
    second2 = to_rings(ha2, hb2, (g22s, g22r), along_z, along_y)
    arrived(second1)
    gf1[mark] = jnp.concatenate([jnp.sum(ha1[...], axis=0), jnp.sum(hb1[...], axis=0)], axis=0)

    over1 = to_all_marks(gf1, fxs, fxr)
    arrived(second2)
    gf2[mark] = jnp.concatenate([jnp.sum(ha2[...], axis=0), jnp.sum(hb2[...], axis=0)], axis=0)
    under = to_all_marks(gf2, f2s, f2r)
    arrived(over1)
    g1[...] = gf1[...].reshape(128, 128)

    psecond = []
    arrived(pfirst)
    started.extend(pfirst)
    asum, bsum = pva[z], pvb[y]
    for d in range(1, RING):
        asum, bsum = asum + pza[d], bsum + pzb[d]
    for q in range(RING):
        psa[q] = asum[4 * q : 4 * q + 4, :]
        psb[q] = bsum[4 * q : 4 * q + 4, :]
    for d in FAR_RING:
        psecond.append(push(psa.at[(y + d) % RING], pya.at[d], y1s.at[0, d - 1], y1r.at[0, d - 1], at_y(d)))
        psecond.append(push(psb.at[(z + d) % RING], pyb.at[d], y1s.at[1, d - 1], y1r.at[1, d - 1], at_z(d)))
    started.extend(psecond)

    one = inverse_factor([g1[8 * g : 8 * g + 8, :] for g in range(16)])
    for g in range(16):
        inv[0, 8 * g : 8 * g + 8, :] = one[g]
    arrived(under)
    g2[...] = gf2[...].reshape(256, 128)
    inv1 = inv[0]
    low = dot_t(g2[0:128, :], inv1)
    g2[128:256, :] = g2[128:256, :] - dot_t(low, low)
    head = dot_t(sketch[:, 0:128], inv1)
    middle = sketch[:, 128:256] - dot_t(head, low)

    def finish_projection():
        arrived(psecond)
        left, right = psa[y], psb[z]
        for d in range(1, RING):
            left, right = left + pya[d], right + pyb[d]
        left = jnp.concatenate([left, left], axis=0)
        right = jnp.concatenate([right, right], axis=0)
        head_p = dot_t(left, inv1)
        loadings_ref[:, 0:128] = head_p[0:4]
        middles.append(right - dot_t(head_p, low))

    middles = [middle]
    two = inverse_factor([g2[128 + 8 * g : 136 + 8 * g, :] for g in range(16)], {10: finish_projection})
    for g in range(16):
        inv[1, 8 * g : 8 * g + 8, :] = two[g]
    inv2 = inv[1]
    tail = dot_t(jnp.concatenate(middles, axis=0), inv2)
    basis_ref[:, 0:128] = math.sqrt(total) * head
    basis_ref[:, 128:256] = math.sqrt(total) * tail[0:64]
    loadings_ref[:, 128:256] = tail[64:68]

    for copy in started:
        copy.wait_send()


def hand_over(basis_in, loadings_in, basis_out, loadings_out, sems):
    copies = [
        pltpu.make_async_copy(basis_in, basis_out, sems.at[0]),
        pltpu.make_async_copy(loadings_in, loadings_out, sems.at[1]),
    ]
    for copy in copies:
        copy.start()
    for copy in copies:
        copy.wait()


def per_device(dosage, alt_count, obs_count, sample_weight, test_matrix):
    total = dosage.shape[0] * lax.axis_size("samp")
    dma = pltpu.SemaphoreType.DMA
    vmem = pl.BlockSpec(memory_space=pltpu.VMEM)
    hbm = pl.BlockSpec(memory_space=pltpu.HBM)
    two_rings = [dma((2, RING - 1))] * 2
    shapes = ((64, 256), F32), ((4, 256), F32)
    args = (
        dosage,
        alt_count.reshape(2, 128),
        obs_count.reshape(2, 128),
        sample_weight.reshape(4, 128),
        test_matrix,
    )
    basis, loadings = pl.pallas_call(
        functools.partial(kernel, total),
        out_shape=tuple(pltpu.VMEM(*s) for s in shapes),
        in_specs=[hbm] * 5,
        out_specs=(vmem, vmem),
        scratch_shapes=[
            pltpu.VMEM((512, 256), BF16),
            pltpu.VMEM((2, 128), jnp.int32),
            pltpu.VMEM((2, 128), jnp.int32),
            pltpu.VMEM((4, 128), F32),
            pltpu.VMEM((512, 256), BF16),
            pltpu.VMEM((RING, RING, 4, 128), BF16),
            pltpu.VMEM((RING, RING, 4, 128), BF16),
            pltpu.VMEM((256, 256), F32),
            pltpu.VMEM((256, 256), BF16),
            pltpu.VMEM((2, MARKS, 64, 128), F32),
            pltpu.VMEM((2, XS, 64, 128), F32),
            pltpu.VMEM((2, XS, 64, 128), F32),
            pltpu.VMEM((2, XS, 64, 128), F32),
            pltpu.VMEM((64, 256), F32),
            *[pltpu.VMEM((MARKS, 64, 128), BF16)] * 2,
            pltpu.VMEM((128, 128), F32),
            pltpu.VMEM((256, 128), F32),
            *[pltpu.VMEM((RING, 8, 128), F32)] * 4,
            pltpu.VMEM((MARKS, 16, 128), F32),
            *[pltpu.VMEM((RING, 16, 128), F32)] * 4,
            pltpu.VMEM((MARKS, 32, 128), F32),
            pltpu.VMEM((2, 128, 128), F32),
            *[pltpu.VMEM((RING, 32, 128), F32)] * 4,
            *[pltpu.VMEM((RING, 4, 128), F32)] * 4,
            pltpu.VMEM((256, 128), F32),
            dma((6,)),
            *two_rings, *two_rings,
            *[dma((2, XS))] * 4,
            *[dma((XS,))] * 4,
            *[dma((MARKS - 1,))] * 2,
            *two_rings, *two_rings, *two_rings, *two_rings,
            *[dma((MARKS - 1,))] * 4,
            *two_rings, *two_rings,
        ],
        compiler_params=pltpu.CompilerParams(
            collective_id=0, has_side_effects=True, vmem_limit_bytes=24 * 1024 * 1024
        ),
    )(*[pltpu.with_memory_space_constraint(arg, pltpu.HBM) for arg in args])
    return pl.pallas_call(
        hand_over,
        out_shape=tuple(jax.ShapeDtypeStruct(*s) for s in shapes),
        in_specs=[vmem] * 2,
        out_specs=(hbm, hbm),
        scratch_shapes=[dma((2,))],
        compiler_params=pltpu.CompilerParams(vmem_limit_bytes=1024 * 1024),
    )(basis, loadings)


def solution(mesh):
    return jax.shard_map(
        per_device,
        mesh=mesh,
        in_specs=(P("samp", "mark"), P("mark"), P("mark"), P("samp"), P(("mark", "samp"), None)),
        out_specs=(P(("samp", "mark"), None), P(("mark", "samp"), None)),
        check_vma=False,
    )
```

```python
import functools
import math

import jax
import jax.numpy as jnp
from jax import lax
from jax.experimental import pallas as pl
from jax.experimental.pallas import tpu as pltpu
from jax.sharding import PartitionSpec as P

F32 = jnp.float32
BF16 = jnp.bfloat16
RING = 8
XS = 4
CORES = 2
MARKS = XS * CORES
FAR_RING = (4, 3, 5, 2, 6, 1, 7)
FAR_X = (2, 1, 3)
HIGHEST = lax.Precision.HIGHEST


def lanes_of(value, k):
    lane = lax.broadcasted_iota(jnp.int32, (8, 128), 1)
    return jnp.broadcast_to(jnp.sum(jnp.where(lane == k, value, 0.0), axis=1, keepdims=True), (8, 128))


def spread(column):
    return jnp.broadcast_to(column, (8, 128))


def inverse_factor(groups, meanwhile=None):
    lane = lax.broadcasted_iota(jnp.int32, (8, 128), 1)
    row = lax.broadcasted_iota(jnp.int32, (8, 128), 0)
    rows = list(groups)
    count = len(rows)
    own = [lanes_of(rows[0], j) for j in range(8)]
    for b in range(count):
        if meanwhile is not None and b in meanwhile:
            meanwhile[b]()
        start = 8 * b
        inside = (lane >= start) & (lane < start + 8)
        cols = {g: [] for g in range(b + 1, count)}
        for j in range(8):
            for g in range(b + 1, count):
                cols[g].append(lanes_of(rows[g], start + j))
        last = b + 1 == count
        following = None if last else [lanes_of(rows[b + 1], start + 8 + j) for j in range(8)]
        theirs = None if last else list(cols[b + 1])
        panel = jnp.where(inside, jnp.where(lane - start == row, 1.0, 0.0), rows[b])
        done = panel
        for k in range(8):
            pivot = spread(own[k][k : k + 1])
            whole = 1.0 / pivot
            line = spread(panel[k : k + 1])
            done = jnp.where(row == k, line * lax.rsqrt(pivot), done)
            normed = line * whole
            panel = jnp.where(row == k, normed, panel - own[k] * normed)
            across = {j: spread(own[j][k : k + 1]) * whole for j in range(k + 1, 8)}
            for j in range(k + 1, 8):
                own[j] = jnp.where(row == k, across[j], own[j] - own[k] * across[j])
            if not last:
                factor = theirs[k]
                for j in range(k + 1, 8):
                    theirs[j] = theirs[j] - factor * across[j]
                scaled = factor * whole
                for j in range(8):
                    following[j] = following[j] - factor * spread(scaled[j : j + 1])
        rows[b] = done
        lines = [spread(panel[k : k + 1]) for k in range(8)]
        for g in range(b + 1, count):
            left = jnp.where(inside, 0.0, rows[g])
            terms = [cols[g][k] * lines[k] for k in range(8)]
            while len(terms) > 1:
                terms = [terms[i] + terms[i + 1] for i in range(0, len(terms), 2)]
            rows[g] = left - terms[0]
        own = following
    return [jnp.where(lane <= row + 8 * g, rows[g], 0.0) for g in range(count)]


def dot_t(a, b):
    return lax.dot_general(a, b, (((1,), (1,)), ((), ())), precision=HIGHEST, preferred_element_type=F32)


def dot_cols(a, b):
    return lax.dot_general(a, b, (((0,), (0,)), ((), ())), preferred_element_type=F32)


def kernel(
    total,
    dosage_hbm, alt_hbm, obs_hbm, weight_hbm, test_hbm,
    basis_ref, loadings_ref,
    dosage, alt, obs, weight, std, ta, tb, tfull, tbf,
    theirs, mine, pair_in, sk_out, sk_in, sketch, yr0, yr1,
    g1, g2, ga1, gb1, ha1, hb1, gf1, ga2, gb2, ha2, hb2, gf2, inv,
    pva, pvb, pza, pzb, psa, psb, pya, pyb, pm,
    in_sem,
    t1s, t1r, t2s, t2r, prs, prr, sks, skr, yxs, yxr, yps, ypr, y2s, y2r,
    g11s, g11r, g12s, g12r, g21s, g21r, g22s, g22r,
    fxs, fxr, f2s, f2r, z1s, z1r, y1s, y1r,
):
    samp, mark = lax.axis_index("samp"), lax.axis_index("mark")
    z, y = samp // RING, samp % RING
    x, c = mark // CORES, mark % CORES
    partner = (samp, x * CORES + (1 - c))

    def at_y(d):
        return (z * RING + (y + d) % RING, mark)

    def at_z(d):
        return (((z + d) % RING) * RING + y, mark)

    def at_x(d):
        return (samp, ((x + d) % XS) * CORES + c)

    def at_other(d):
        return (samp, ((x + d) % XS) * CORES + (1 - c))

    def push(src, dst, send, recv, to):
        copy = pltpu.make_async_remote_copy(
            src_ref=src, dst_ref=dst, send_sem=send, recv_sem=recv,
            device_id=to, device_id_type=pl.DeviceIdType.MESH,
        )
        copy.start()
        return copy

    started = []

    own_a = pltpu.make_async_copy(test_hbm.at[:, pl.ds(0, 128)], ta.at[z, y], in_sem.at[0])
    own_b = pltpu.make_async_copy(test_hbm.at[:, pl.ds(128, 128)], tb.at[y, z], in_sem.at[1])
    rest = [
        pltpu.make_async_copy(src, dst, in_sem.at[2 + i])
        for i, (src, dst) in enumerate(
            ((dosage_hbm, dosage), (alt_hbm, alt), (obs_hbm, obs), (weight_hbm, weight))
        )
    ]
    own_a.start()
    own_b.start()
    for copy in rest:
        copy.start()

    barrier = pltpu.get_barrier_semaphore()
    peers = [at_y(d) for d in FAR_RING] + [at_z(d) for d in FAR_RING] + [at_x(d) for d in FAR_X]
    peers += [at_other(d) for d in FAR_X] + [partner]
    for peer in peers:
        pl.semaphore_signal(barrier, inc=1, device_id=peer, device_id_type=pl.DeviceIdType.MESH)
    own_a.wait()
    own_b.wait()
    pl.semaphore_wait(barrier, len(peers))

    first = []
    for d in FAR_RING:
        first.append(push(ta.at[z, y], ta.at[z, y], t1s.at[0, d - 1], t1r.at[0, d - 1], at_y(d)))
        first.append(push(tb.at[y, z], tb.at[y, z], t1s.at[1, d - 1], t1r.at[1, d - 1], at_z(d)))

    for copy in rest:
        copy.wait()
    freq = alt[...].astype(F32) / (2.0 * obs[...].astype(F32))
    scale = 1.0 / jnp.sqrt(2.0 * freq * (1.0 - freq))
    roots = jnp.sqrt(weight[...])
    tall = jnp.concatenate([roots] * 2, axis=0).T
    for q in range(4):
        rows = pl.ds(128 * q, 128)
        weights = jnp.broadcast_to(tall[:, q : q + 1], (128, 128))
        for h in range(2):
            cols = pl.ds(128 * h, 128)
            centred = dosage[rows, cols].astype(F32) - 2.0 * freq[h : h + 1]
            std[rows, cols] = (weights * centred * scale[h : h + 1]).astype(BF16)

    for copy in first:
        copy.wait_recv()
    second = []
    for d in FAR_RING:
        second.append(push(ta.at[z], ta.at[z], t2s.at[0, d - 1], t2r.at[0, d - 1], at_z(d)))
        second.append(push(tb.at[y], tb.at[y], t2s.at[1, d - 1], t2r.at[1, d - 1], at_y(d)))
    for copy in second:
        copy.wait_recv()
    started += first + second
    for s in range(RING * RING):
        tfull[4 * s : 4 * s + 4, 0:128] = ta[s // RING, s % RING].astype(F32)
        tfull[4 * s : 4 * s + 4, 128:256] = tb[s % RING, s // RING].astype(F32)
    tbf[...] = tfull[...].astype(BF16)

    def block(d, core):
        return ((x + d) % XS) * CORES + core

    def products(core, h):
        blocks = [std[pl.ds(pl.multiple_of(block(d, core) * 64, 64), 64), :] for d in (2, 1, 3, 0)]
        return jnp.dot(
            jnp.concatenate(blocks, axis=0), tbf[:, 128 * h : 128 * h + 128], preferred_element_type=F32
        )

    steps = [(h, d) for h in range(2) for d in (2, 1, 3, 0)]
    place = {2: 0, 1: 1, 3: 2, 0: 3}
    pair, along = {}, {}
    for h in range(2):
        theirs[h] = products(1 - c, h).reshape(XS, 64, 128)
        for d in (2, 1, 3, 0):
            pair[h, d] = push(theirs.at[h, place[d]], pair_in.at[h, d], prs.at[h, d], prr.at[h, d], partner)
    for h in range(2):
        mine[h] = products(c, h).reshape(XS, 64, 128)
    for h, d in steps:
        if d:
            pair[h, d].wait_recv()
            sk_out[h, d] = mine[h, place[d]] + pair_in[h, d]
            along[h, d] = push(sk_out.at[h, d], sk_in.at[h, d], sks.at[h, d], skr.at[h, d], at_x(d))
    started += list(pair.values()) + list(along.values())

    def own_half(h):
        pair[h, 0].wait_recv()
        value = mine[h, place[0]] + pair_in[h, 0]
        for d in (1, 3, 2):
            along[h, d].wait_recv()
            value = value + sk_in[h, d]
        sketch[:, 128 * h : 128 * h + 128] = value
        return value.astype(BF16)

    def to_all_marks(buf, sends, recvs):
        copies = [
            push(buf.at[mark], buf.at[mark], sends.at[k], recvs.at[k], to)
            for k, to in enumerate([at_other(d) for d in FAR_X] + [at_x(d) for d in FAR_X] + [partner])
        ]
        started.extend(copies)
        return copies

    yr0[mark] = own_half(0)
    out = {d: push(yr0.at[mark], yr0.at[mark], yxs.at[d], yxr.at[d], at_x(d)) for d in FAR_X}
    over = {0: push(yr0.at[mark], yr0.at[mark], yps.at[0], ypr.at[0], partner)}
    yr1[mark] = own_half(1)
    second_half = to_all_marks(yr1, y2s, y2r)
    for d in (1, 3, 2):
        out[d].wait_recv()
        slot = ((x + XS - d) % XS) * CORES + c
        over[d] = push(yr0.at[slot], yr0.at[slot], yps.at[d], ypr.at[d], partner)
    for d in (0, 1, 3, 2):
        over[d].wait_recv()
    started += list(out.values()) + list(over.values())

    rounded0 = yr0[...].reshape(512, 128)

    def to_rings(left, right, sems, there, back):
        (lslot, lto), (rslot, rto) = there, back
        copies = []
        for d in FAR_RING:
            copies.append(push(left.at[lslot], left.at[lslot], sems[0].at[0, d - 1], sems[1].at[0, d - 1], lto(d)))
            copies.append(push(right.at[rslot], right.at[rslot], sems[0].at[1, d - 1], sems[1].at[1, d - 1], rto(d)))
        started.extend(copies)
        return copies

    def arrived(copies):
        for copy in copies:
            copy.wait_recv()

    along_y, along_z = (y, at_y), (z, at_z)

    g1[...] = dot_cols(rounded0, rounded0)
    part = pl.multiple_of(mark * 16, 16)
    ga1[y] = g1[pl.ds(part, 8), :]
    gb1[z] = g1[pl.ds(pl.multiple_of(part + 8, 8), 8), :]
    first1 = to_rings(ga1, gb1, (g11s, g11r), along_y, along_z)
    arrived(second_half)
    rounded1 = yr1[...].reshape(512, 128)
    g2[0:128, :] = dot_cols(rounded1, rounded0)
    g2[128:256, :] = dot_cols(rounded1, rounded1)
    part = pl.multiple_of(mark * 32, 32)
    ga2[y] = g2[pl.ds(part, 16), :]
    gb2[z] = g2[pl.ds(pl.multiple_of(part + 16, 16), 16), :]
    first2 = to_rings(ga2, gb2, (g12s, g12r), along_y, along_z)

    pva[...] = dot_cols(std[...], rounded0).reshape(RING, 32, 128)
    pm[...] = dot_cols(std[...], rounded1)
    for q in range(RING * RING):
        pvb[q % RING, 4 * (q // RING) : 4 * (q // RING) + 4, :] = pm[4 * q : 4 * q + 4, :]

    pfirst = []

    def pass_on(distances):
        for d in distances:
            pfirst.append(push(pva.at[(z + d) % RING], pza.at[d], z1s.at[0, d - 1], z1r.at[0, d - 1], at_z(d)))
            pfirst.append(push(pvb.at[(y + d) % RING], pzb.at[d], z1s.at[1, d - 1], z1r.at[1, d - 1], at_y(d)))

    pass_on((3, 5, 2, 6, 1, 7))
    arrived(first1)
    ha1[z] = jnp.sum(ga1[...], axis=0)
    hb1[y] = jnp.sum(gb1[...], axis=0)
    second1 = to_rings(ha1, hb1, (g21s, g21r), along_z, along_y)
    pass_on((4,))
    arrived(first2)
    ha2[z] = jnp.sum(ga2[...], axis=0)
    hb2[y] = jnp.sum(gb2[...], axis=0)
    second2 = to_rings(ha2, hb2, (g22s, g22r), along_z, along_y)
    arrived(second1)
    gf1[mark] = jnp.concatenate([jnp.sum(ha1[...], axis=0), jnp.sum(hb1[...], axis=0)], axis=0)

    over1 = to_all_marks(gf1, fxs, fxr)
    arrived(second2)
    gf2[mark] = jnp.concatenate([jnp.sum(ha2[...], axis=0), jnp.sum(hb2[...], axis=0)], axis=0)
    under = to_all_marks(gf2, f2s, f2r)
    drained = len(started)
    for copy in started[: drained - 2 * (MARKS - 1)]:
        copy.wait_send()
    arrived(over1)
    g1[...] = gf1[...].reshape(128, 128)

    psecond = []
    arrived(pfirst)
    started.extend(pfirst)
    asum, bsum = pva[z], pvb[y]
    for d in range(1, RING):
        asum, bsum = asum + pza[d], bsum + pzb[d]
    for q in range(RING):
        psa[q] = asum[4 * q : 4 * q + 4, :]
        psb[q] = bsum[4 * q : 4 * q + 4, :]
    for d in FAR_RING:
        psecond.append(push(psa.at[(y + d) % RING], pya.at[d], y1s.at[0, d - 1], y1r.at[0, d - 1], at_y(d)))
        psecond.append(push(psb.at[(z + d) % RING], pyb.at[d], y1s.at[1, d - 1], y1r.at[1, d - 1], at_z(d)))
    started.extend(psecond)

    one = inverse_factor([g1[8 * g : 8 * g + 8, :] for g in range(16)])
    for g in range(16):
        inv[0, 8 * g : 8 * g + 8, :] = one[g]
    arrived(under)
    g2[...] = gf2[...].reshape(256, 128)
    inv1 = inv[0]
    low = dot_t(g2[0:128, :], inv1)
    g2[128:256, :] = g2[128:256, :] - dot_t(low, low)
    head = dot_t(sketch[:, 0:128], inv1)
    middle = sketch[:, 128:256] - dot_t(head, low)

    def finish_projection():
        arrived(psecond)
        left, right = psa[y], psb[z]
        for d in range(1, RING):
            left, right = left + pya[d], right + pyb[d]
        left = jnp.concatenate([left, left], axis=0)
        right = jnp.concatenate([right, right], axis=0)
        head_p = dot_t(left, inv1)
        loadings_ref[:, 0:128] = head_p[0:4]
        middles.append(right - dot_t(head_p, low))

    middles = [middle]
    two = inverse_factor([g2[128 + 8 * g : 136 + 8 * g, :] for g in range(16)], {10: finish_projection})
    for g in range(16):
        inv[1, 8 * g : 8 * g + 8, :] = two[g]
    inv2 = inv[1]
    tail = dot_t(jnp.concatenate(middles, axis=0), inv2)
    basis_ref[:, 0:128] = math.sqrt(total) * head
    basis_ref[:, 128:256] = math.sqrt(total) * tail[0:64]
    loadings_ref[:, 128:256] = tail[64:68]

    for copy in started[drained - 2 * (MARKS - 1) :]:
        copy.wait_send()


def hand_over(basis_in, loadings_in, basis_out, loadings_out, sems):
    copies = [
        pltpu.make_async_copy(basis_in, basis_out, sems.at[0]),
        pltpu.make_async_copy(loadings_in, loadings_out, sems.at[1]),
    ]
    for copy in copies:
        copy.start()
    for copy in copies:
        copy.wait()


def per_device(dosage, alt_count, obs_count, sample_weight, test_matrix):
    total = dosage.shape[0] * lax.axis_size("samp")
    dma = pltpu.SemaphoreType.DMA
    vmem = pl.BlockSpec(memory_space=pltpu.VMEM)
    hbm = pl.BlockSpec(memory_space=pltpu.HBM)
    two_rings = [dma((2, RING - 1))] * 2
    shapes = ((64, 256), F32), ((4, 256), F32)
    args = (
        dosage,
        alt_count.reshape(2, 128),
        obs_count.reshape(2, 128),
        sample_weight.reshape(4, 128),
        test_matrix,
    )
    basis, loadings = pl.pallas_call(
        functools.partial(kernel, total),
        out_shape=tuple(pltpu.VMEM(*s) for s in shapes),
        in_specs=[hbm] * 5,
        out_specs=(vmem, vmem),
        scratch_shapes=[
            pltpu.VMEM((512, 256), BF16),
            pltpu.VMEM((2, 128), jnp.int32),
            pltpu.VMEM((2, 128), jnp.int32),
            pltpu.VMEM((4, 128), F32),
            pltpu.VMEM((512, 256), BF16),
            pltpu.VMEM((RING, RING, 4, 128), BF16),
            pltpu.VMEM((RING, RING, 4, 128), BF16),
            pltpu.VMEM((256, 256), F32),
            pltpu.VMEM((256, 256), BF16),
            *[pltpu.VMEM((2, XS, 64, 128), F32)] * 2,
            pltpu.VMEM((2, XS, 64, 128), F32),
            pltpu.VMEM((2, XS, 64, 128), F32),
            pltpu.VMEM((2, XS, 64, 128), F32),
            pltpu.VMEM((64, 256), F32),
            *[pltpu.VMEM((MARKS, 64, 128), BF16)] * 2,
            pltpu.VMEM((128, 128), F32),
            pltpu.VMEM((256, 128), F32),
            *[pltpu.VMEM((RING, 8, 128), F32)] * 4,
            pltpu.VMEM((MARKS, 16, 128), F32),
            *[pltpu.VMEM((RING, 16, 128), F32)] * 4,
            pltpu.VMEM((MARKS, 32, 128), F32),
            pltpu.VMEM((2, 128, 128), F32),
            *[pltpu.VMEM((RING, 32, 128), F32)] * 4,
            *[pltpu.VMEM((RING, 4, 128), F32)] * 4,
            pltpu.VMEM((256, 128), F32),
            dma((6,)),
            *two_rings, *two_rings,
            *[dma((2, XS))] * 4,
            *[dma((XS,))] * 4,
            *[dma((MARKS - 1,))] * 2,
            *two_rings, *two_rings, *two_rings, *two_rings,
            *[dma((MARKS - 1,))] * 4,
            *two_rings, *two_rings,
        ],
        compiler_params=pltpu.CompilerParams(
            collective_id=0, has_side_effects=True, vmem_limit_bytes=24 * 1024 * 1024
        ),
    )(*[pltpu.with_memory_space_constraint(arg, pltpu.HBM) for arg in args])
    return pl.pallas_call(
        hand_over,
        out_shape=tuple(jax.ShapeDtypeStruct(*s) for s in shapes),
        in_specs=[vmem] * 2,
        out_specs=(hbm, hbm),
        scratch_shapes=[dma((2,))],
        compiler_params=pltpu.CompilerParams(vmem_limit_bytes=1024 * 1024),
    )(basis, loadings)


def solution(mesh):
    return jax.shard_map(
        per_device,
        mesh=mesh,
        in_specs=(P("samp", "mark"), P("mark"), P("mark"), P("samp"), P(("mark", "samp"), None)),
        out_specs=(P(("samp", "mark"), None), P(("mark", "samp"), None)),
        check_vma=False,
    )
```
